32 devices in a mesh: rows: 8 (over z, x), rep: 4 (over y, core).
Axes of the slice: x: 2, y: 2, z: 4, core: 2. Of those that a mesh axis runs over, the one named last changes fastest.
Arguments:
- requests: int32 [32, 8, 128], P(('rows', 'rep')), may hold values from 0 to 1023
- request_counts: int32 [32, 8], P(('rows', 'rep')), may hold values from 0 to 128, as said below
- table: bfloat16 [8192, 512], P('rows')
- gain: float32 [512], replicated, may hold values from 0.5 to 1.5
Outputs:
- normalized: bfloat16 [32, 8, 128, 512], P(('rows', 'rep'))
- row_counts: int32 [8192], P('rows')
- moments: float32 [2, 2], replicated
The draws below stay inside these ranges and needn't reach their ends.
Inputs may be any that keep to these rules, and one draw needn't show every extreme that they name: Each device uses request_counts[d, o] of its 128 slots toward owner o; in every draw one owner's slots are full from every device.
All inputs are finite; a program needn't handle non-finite values.
Results may differ from the reference program's by a relative error of at most 0.0004.
Values may be sent and summed in bfloat16 or wider, within the bound.
No kernel may reach another device: no remote copies, remote signals or barrier semaphores. Data moves between devices by JAX's collectives and lax.ppermute only.
A program may use at most 64 MiB of HBM per device.

```python
import math
import jax
import jax.numpy as jnp
import numpy as np
from jax import lax

WIDTH = 256
LAYERS = 2
ROWS_DEV = 1024
VOCAB = 8192
CAP = 128
N_ROWS = 8
DEVICES = 32


def draw_request_counts(key, part):
    first, second, third, fourth = jax.random.split(jax.random.fold_in(key, 11), 4)
    level = jax.random.randint(first, (1, N_ROWS), CAP // 2, CAP + 1)
    hottest = jax.random.randint(second, (), 0, N_ROWS)
    bits_one = jax.random.randint(third, (DEVICES, N_ROWS), 0, 1048576)
    bits_two = jax.random.randint(fourth, (DEVICES, N_ROWS), 0, 1048576)
    picked = jnp.maximum(bits_one % (level + 1), bits_two % (level + 1))
    full_owner = jnp.arange(N_ROWS)[None, :] == hottest
    return jnp.where(full_owner, CAP, picked).astype(jnp.int32)


def draw_table(key, part):
    first, second, third = jax.random.split(jax.random.fold_in(key, 23), 3)
    position = jnp.arange(VOCAB, dtype=jnp.float32) / VOCAB
    row_scale = jnp.exp(jax.random.uniform(second, (VOCAB, 1), jnp.float32, 0.0, math.log(10.0)))
    row_scale = row_scale * (1.0 + 2.0 * position)[:, None]
    col_scale = jnp.exp(jax.random.uniform(third, (1, LAYERS * WIDTH), jnp.float32, math.log(0.5), math.log(2.0)))
    values = jax.random.normal(first, (VOCAB, LAYERS * WIDTH), jnp.float32) * row_scale * col_scale
    return values.astype(jnp.bfloat16)


def set_ends(values, key, low, largest):
    shape = values.shape
    place = [jax.random.randint(jax.random.fold_in(key, axis), (), 0, shape[axis]) for axis in range(len(shape))]
    values = values.at[tuple(place)].set(low)
    longest = shape.index(max(shape))
    place[longest] = (place[longest] + 1) % shape[longest]
    return values.at[tuple(place)].set(largest)


def rank_bounds(count, slope):
    portions = [(1 << 20) // math.isqrt(standing ** slope) + 1 for standing in range(1, count + 1)]
    spread = 1 + sum(portions) // (1 << 30)
    return np.cumsum(np.array([max(1, weight // spread) for weight in portions]))


def ranked_ids(key, shape, count, skew):
    grid = rank_bounds(count, skew)
    lot = jax.random.randint(jax.random.fold_in(key, 1), shape, 0, int(grid[count - 1]))
    rank = jnp.searchsorted(jnp.asarray(grid, jnp.int32), lot, side="right")
    return jax.random.permutation(jax.random.fold_in(key, 2), count)[rank].astype(jnp.int32)


def setup_inputs(seed: int = 0) -> dict:
    key_list = jax.random.split(jax.random.key(seed), 5)
    requests = set_ends(ranked_ids(key_list[0], (DEVICES, N_ROWS, CAP), ROWS_DEV, 2), jax.random.fold_in(key_list[0], 3), 0, ROWS_DEV - 1).astype(jnp.int32)
    request_counts = draw_request_counts(jax.random.fold_in(key_list[4], 71), 0)
    table = draw_table(jax.random.fold_in(key_list[4], 71), 0)
    gain = jnp.clip(1.0 + 0.1 * jax.random.normal(key_list[3], (LAYERS * WIDTH,), jnp.float32), 0.5, 1.5)
    return dict(requests=requests, request_counts=request_counts, table=table, gain=gain)


epsilon = 1e-06

def reference(requests, request_counts, table, gain):
    offsets = (jnp.arange(N_ROWS, dtype=jnp.int32) * ROWS_DEV)[None, :, None]
    global_index = (requests + offsets).astype(jnp.int32)
    slot_index = jnp.arange(CAP, dtype=jnp.int32)[None, None, :]
    live_slot = slot_index < request_counts[:, :, None]
    row_counts = jnp.zeros((VOCAB,), jnp.int32).at[global_index.reshape(-1)].add(live_slot.reshape(-1).astype(jnp.int32))
    shaped = table.astype(jnp.float32).reshape(VOCAB, LAYERS, WIDTH)
    weights = row_counts.astype(jnp.float32)
    entries = jnp.sum(weights) * WIDTH
    layer_mean = jnp.dot(weights, lax.optimization_barrier(jnp.sum(shaped, axis=2)), precision=lax.Precision.HIGHEST) / entries
    centered = lax.optimization_barrier(jnp.sum(jnp.square(shaped - layer_mean[None, :, None]), axis=2))
    layer_var = jnp.dot(weights, centered, precision=lax.Precision.HIGHEST) / entries
    inverse = jnp.repeat(lax.rsqrt(layer_var + epsilon), WIDTH) * gain
    mean_full = jnp.repeat(layer_mean, WIDTH)

    def one_device(pair):
        index_rows, live_rows = pair
        fetched = jnp.take(table, index_rows.reshape(-1), axis=0).astype(jnp.float32)
        scaled = (fetched - mean_full) * inverse
        scaled = jnp.where(live_rows.reshape(-1, 1), scaled, jnp.zeros_like(scaled))
        return scaled.reshape(N_ROWS, CAP, LAYERS * WIDTH).astype(jnp.bfloat16)
    normalized = lax.map(one_device, (global_index, live_slot))
    return (normalized, row_counts, jnp.stack([layer_mean, layer_var]))
```

```python
import functools

import jax
import jax.numpy as jnp
from jax import lax
from jax.experimental import pallas as pl
from jax.experimental.pallas import tpu as pltpu
from jax.sharding import PartitionSpec as P

WIDTH = 256
LAYERS = 2
LANES = 128
SUBLANES = 8

epsilon = 1e-06


def row_moments_kernel(table_ref, moments_ref):
    blocks = table_ref.shape[0] // LANES
    lane = lax.broadcasted_iota(jnp.int32, (LANES, LANES), 1)
    columns = jnp.zeros((LANES, LANES), jnp.float32)
    for block in range(blocks):
        for layer in range(LAYERS):
            x = table_ref[
                block * LANES : (block + 1) * LANES, layer * WIDTH : (layer + 1) * WIDTH
            ].astype(jnp.float32)
            mean = jnp.sum(x, axis=1, keepdims=True) * (1.0 / WIDTH)
            square = jnp.sum(jnp.square(x - mean), axis=1, keepdims=True)
            columns = jnp.where(lane == layer * blocks + block, mean, columns)
            columns = jnp.where(lane == (LAYERS + layer) * blocks + block, square, columns)
    moments_ref[...] = jnp.transpose(columns)[: 2 * LAYERS * blocks]


def serve_kernel(slot_count, mine_ref, wanted_ref, moments_ref, table_ref, payload_ref, counts_ref, high_ref, low_ref):
    held_rows, columns = table_ref.shape
    blocks = held_rows // LANES
    requests = wanted_ref.shape[0]
    lane = lax.broadcasted_iota(jnp.int32, (LANES, LANES), 1)
    block_row = lax.broadcasted_iota(jnp.int32, (blocks, LANES), 0)
    one, nought = jnp.bfloat16(1), jnp.bfloat16(0)

    wanted = wanted_ref[...]
    upright = jnp.transpose(wanted)
    for row in range(requests):
        span = slice(row * LANES, (row + 1) * LANES)
        high = wanted[row : row + 1] // LANES
        low = upright[:, row : row + 1] % LANES
        high_ref[:, span] = jnp.where(block_row == high, 1.0, 0.0).astype(jnp.bfloat16)
        low_ref[span, :] = jnp.where(lane == low, 1.0, 0.0).astype(jnp.bfloat16)
    weights = jnp.dot(high_ref[...], low_ref[...], preferred_element_type=jnp.float32)
    counts_ref[...] = weights.astype(jnp.int32)

    tile_row = lax.broadcasted_iota(jnp.int32, (SUBLANES, LANES), 0)
    tile_lane = lax.broadcasted_iota(jnp.int32, (SUBLANES, LANES), 1)

    def total(a):
        return jnp.sum(jnp.sum(a, axis=1, keepdims=True), axis=0, keepdims=True)

    count = total(weights)
    figures = jnp.where(tile_lane == 0, count, 0.0)
    for layer in range(LAYERS):
        row_mean = moments_ref[layer * blocks : (layer + 1) * blocks]
        row_square = moments_ref[(LAYERS + layer) * blocks : (LAYERS + layer + 1) * blocks]
        mean = total(weights * row_mean) / jnp.maximum(count, 1.0)
        square = total(weights * (row_square + WIDTH * jnp.square(row_mean - mean)))
        figures = jnp.where(tile_lane == 1 + layer, mean, figures)
        figures = jnp.where(tile_lane == 1 + LAYERS + layer, square, figures)
    first = figures.astype(jnp.bfloat16).astype(jnp.float32)
    second = (figures - first).astype(jnp.bfloat16).astype(jnp.float32)
    third = figures - first - second
    terms = jnp.where(tile_row == 0, first, jnp.where(tile_row == 1, second, third)).astype(jnp.bfloat16)

    pieces = columns // LANES
    owned = mine_ref.shape[0]
    peers = payload_ref.shape[0]
    mine = jnp.transpose(mine_ref[...])
    row_lane = lax.broadcasted_iota(jnp.int32, (LANES, held_rows), 1)
    for row in range(owned):
        chosen = jnp.where(row_lane == mine[:, row : row + 1], 1.0, 0.0).astype(jnp.bfloat16)
        rows = jnp.dot(chosen, table_ref[...], preferred_element_type=jnp.float32)
        for start in range(0, LANES, slot_count):
            peer = (row * LANES + start) // slot_count
            for piece in range(pieces):
                payload_ref[peer, piece * slot_count : (piece + 1) * slot_count, :] = rows[
                    start : start + slot_count, piece * LANES : (piece + 1) * LANES
                ].astype(jnp.bfloat16)
    for peer in range(peers):
        payload_ref[peer, pieces * slot_count :, :] = terms


def normalize_kernel(used_ref, received_ref, gain_ref, out_ref, moments_ref, ready_ref, sems):
    owners, slot_count, columns = out_ref.shape
    pieces = columns // LANES
    count = jnp.zeros((1, LANES), jnp.float32)
    tail = [
        received_ref[owner, pieces * slot_count :, :].astype(jnp.float32) for owner in range(owners)
    ]
    figures = [t[0:1] + t[1:2] + t[2:3] for t in tail]
    counts = [f[:, 0:1] for f in figures]
    entries = functools.reduce(jnp.add, counts)
    out_row = lax.broadcasted_iota(jnp.int32, moments_ref.shape, 0)
    out_lane = lax.broadcasted_iota(jnp.int32, moments_ref.shape, 1)
    summary = jnp.zeros(moments_ref.shape, jnp.float32)
    means, scales = [], []
    for layer in range(LAYERS):
        held = [f[:, 1 + layer : 2 + layer] for f in figures]
        squares = [f[:, 1 + LAYERS + layer : 2 + LAYERS + layer] for f in figures]
        mean = functools.reduce(jnp.add, [c * m for c, m in zip(counts, held)]) / entries
        square = functools.reduce(
            jnp.add, [s + WIDTH * c * jnp.square(m - mean) for c, m, s in zip(counts, held, squares)]
        )
        variance = square / (entries * WIDTH)
        means.append(mean)
        scales.append(lax.rsqrt(variance + epsilon))
        summary = jnp.where(out_lane == layer, jnp.where(out_row == 0, mean, variance), summary)
    moments_ref[...] = summary

    slot = lax.broadcasted_iota(jnp.int32, (slot_count, LANES), 0)
    copies = []
    for owner in range(owners):
        live = slot < used_ref[0, owner]
        for piece in range(pieces):
            span = slice(piece * LANES, (piece + 1) * LANES)
            layer = piece * LANES // WIDTH
            x = received_ref[owner, piece * slot_count : (piece + 1) * slot_count, :].astype(jnp.float32)
            scaled = (x - means[layer]) * (scales[layer] * gain_ref[:, span])
            ready_ref[owner, :, span] = jnp.where(live, scaled, 0.0).astype(jnp.bfloat16)
        copy = pltpu.make_async_copy(ready_ref.at[owner], out_ref.at[owner], sems.at[owner])
        copy.start()
        copies.append(copy)
    for copy in copies:
        copy.wait()


def per_device(groups, requests, request_counts, table, gain):
    _, owners, slot_count = requests.shape
    held_rows, columns = table.shape
    pieces = columns // LANES
    vmem = pl.BlockSpec(memory_space=pltpu.VMEM)
    slot = lax.broadcasted_iota(jnp.int32, (owners, slot_count), 1)
    asked = jnp.where(slot < request_counts[0][:, None], requests[0], held_rows)
    asked = jnp.broadcast_to(asked[None], (groups, owners, slot_count)).reshape(groups * owners, slot_count)
    wanted = lax.all_to_all(asked, ("rep", "rows"), split_axis=0, concat_axis=0, tiled=True)
    wanted = wanted.reshape(groups, owners * slot_count // LANES, LANES)
    mine = lax.dynamic_index_in_dim(wanted, lax.axis_index("rep"), 0, False)
    wanted = wanted.reshape(-1, LANES)
    blocks = held_rows // LANES
    moments = pl.pallas_call(
        row_moments_kernel,
        out_shape=jax.ShapeDtypeStruct((2 * LAYERS * blocks, LANES), jnp.float32),
        in_specs=[vmem],
        out_specs=vmem,
        name="row_moments",
    )(table)
    payload, row_counts = pl.pallas_call(
        functools.partial(serve_kernel, slot_count),
        out_shape=(
            jax.ShapeDtypeStruct((owners, pieces * slot_count + SUBLANES, LANES), jnp.bfloat16),
            jax.ShapeDtypeStruct((blocks, LANES), jnp.int32),
        ),
        in_specs=[vmem] * 4,
        out_specs=(vmem, vmem),
        scratch_shapes=[
            pltpu.VMEM((blocks, wanted.size), jnp.bfloat16),
            pltpu.VMEM((wanted.size, LANES), jnp.bfloat16),
        ],
        name="serve",
    )(mine, wanted, moments, table)
    received = lax.all_to_all(payload, "rows", split_axis=0, concat_axis=0, tiled=True)
    normalized, summary = pl.pallas_call(
        normalize_kernel,
        out_shape=(
            jax.ShapeDtypeStruct((owners, slot_count, columns), jnp.bfloat16),
            jax.ShapeDtypeStruct((2, LAYERS), jnp.float32),
        ),
        in_specs=[pl.BlockSpec(memory_space=pltpu.SMEM), vmem, vmem],
        out_specs=(pl.BlockSpec(memory_space=pl.ANY), vmem),
        scratch_shapes=[
            pltpu.VMEM((owners, slot_count, columns), jnp.bfloat16),
            pltpu.SemaphoreType.DMA((owners,)),
        ],
        name="normalize",
    )(request_counts, received, gain[None])
    return (normalized[None], row_counts.reshape(-1), summary)


def solution(mesh):
    return jax.shard_map(
        functools.partial(per_device, mesh.shape["rep"]),
        mesh=mesh,
        in_specs=(P(("rows", "rep"), None, None), P(("rows", "rep"), None), P("rows", None), P()),
        out_specs=(P(("rows", "rep"), None, None, None), P("rows"), P()),
        check_vma=False,
    )
```

```python
import functools

import jax
import jax.numpy as jnp
from jax import lax
from jax.experimental import pallas as pl
from jax.experimental.pallas import tpu as pltpu
from jax.sharding import PartitionSpec as P

WIDTH = 256
LAYERS = 2
LANES = 128
SUBLANES = 8
GRANT = 16 << 20
MOST_PERMUTES = 16

epsilon = 1e-06


VMEM = pl.BlockSpec(memory_space=pltpu.VMEM)
SMEM = pl.BlockSpec(memory_space=pltpu.SMEM)
PLACED = pl.BlockSpec(memory_space=pl.ANY)


def total(a):
    return jnp.sum(jnp.sum(a, axis=1, keepdims=True), axis=0, keepdims=True)


def one_hot(match):
    return jnp.where(match, 1.0, 0.0).astype(jnp.bfloat16)


def kernel_call(body, name, out_shape, in_specs, out_specs, scratch=()):
    return pl.pallas_call(
        body,
        name=name,
        out_shape=out_shape,
        in_specs=in_specs,
        out_specs=out_specs,
        scratch_shapes=list(scratch),
        compiler_params=pltpu.CompilerParams(vmem_limit_bytes=GRANT),
    )


def row_moments_kernel(table_ref, moments_ref):
    blocks = table_ref.shape[0] // LANES
    lane = lax.broadcasted_iota(jnp.int32, (LANES, LANES), 1)
    columns = jnp.zeros((LANES, LANES), jnp.float32)
    for block in range(blocks):
        for layer in range(LAYERS):
            x = table_ref[
                block * LANES : (block + 1) * LANES, layer * WIDTH : (layer + 1) * WIDTH
            ].astype(jnp.float32)
            mean = jnp.sum(x, axis=1, keepdims=True) * (1.0 / WIDTH)
            square = jnp.sum(jnp.square(x - mean), axis=1, keepdims=True)
            columns = jnp.where(lane == layer * blocks + block, mean, columns)
            columns = jnp.where(lane == (LAYERS + layer) * blocks + block, square, columns)
    moments_ref[...] = jnp.transpose(columns)[: 2 * LAYERS * blocks]


def ask_kernel(held_rows, groups, used_ref, requests_ref, asked_ref):
    owners, slot_count = requests_ref.shape
    row = lax.broadcasted_iota(jnp.int32, (owners, slot_count), 0)
    slot = lax.broadcasted_iota(jnp.int32, (owners, slot_count), 1)
    used = jnp.zeros((owners, slot_count), jnp.int32)
    for owner in range(owners):
        used = jnp.where(row == owner, used_ref[0, owner], used)
    asked = jnp.where(slot < used, requests_ref[...], held_rows)
    for group in range(groups):
        asked_ref[group * owners : (group + 1) * owners, :] = asked


def tally(wanted, moments_ref, high_ref, low_ref, counts_ref):
    blocks = counts_ref.shape[0]
    lane = lax.broadcasted_iota(jnp.int32, (LANES, LANES), 1)
    block_row = lax.broadcasted_iota(jnp.int32, (blocks, LANES), 0)
    upright = jnp.transpose(wanted)
    for row in range(wanted.shape[0]):
        span = slice(row * LANES, (row + 1) * LANES)
        high_ref[:, span] = one_hot(block_row == wanted[row : row + 1] // LANES)
        low_ref[span, :] = one_hot(lane == upright[:, row : row + 1] % LANES)
    weights = jnp.dot(high_ref[...], low_ref[...], preferred_element_type=jnp.float32)
    counts_ref[...] = weights.astype(jnp.int32)

    tile_row = lax.broadcasted_iota(jnp.int32, (SUBLANES, LANES), 0)
    tile_lane = lax.broadcasted_iota(jnp.int32, (SUBLANES, LANES), 1)
    count = total(weights)
    figures = jnp.where(tile_lane == 0, count, 0.0)
    for layer in range(LAYERS):
        row_mean = moments_ref[layer * blocks : (layer + 1) * blocks]
        row_square = moments_ref[(LAYERS + layer) * blocks : (LAYERS + layer + 1) * blocks]
        mean = total(weights * row_mean) / jnp.maximum(count, 1.0)
        square = total(weights * (row_square + WIDTH * jnp.square(row_mean - mean)))
        figures = jnp.where(tile_lane == 1 + layer, mean, figures)
        figures = jnp.where(tile_lane == 1 + LAYERS + layer, square, figures)
    first = figures.astype(jnp.bfloat16).astype(jnp.float32)
    second = (figures - first).astype(jnp.bfloat16).astype(jnp.float32)
    third = figures - first - second
    return jnp.where(tile_row == 0, first, jnp.where(tile_row == 1, second, third)).astype(jnp.bfloat16)


def pick(table_ref, column):
    lane = lax.broadcasted_iota(jnp.int32, (LANES, table_ref.shape[0]), 1)
    return jnp.dot(one_hot(lane == column), table_ref[...], preferred_element_type=jnp.float32).astype(jnp.bfloat16)


def put(message_ref, rows, terms):
    count, columns = rows.shape
    pieces = columns // LANES
    for piece in range(pieces):
        message_ref[piece * count : (piece + 1) * count, :] = rows[:, piece * LANES : (piece + 1) * LANES]
    message_ref[pieces * count :, :] = terms


def asked_of_me(owners, wanted_ref, shifts):
    me, group = lax.axis_index("rows"), lax.axis_index("rep")
    rows = [wanted_ref[pl.ds(group * owners + lax.rem(me + shift, owners), 1), :] for shift in shifts]
    filler = [rows[0]] * (-len(rows) % SUBLANES)
    return jnp.transpose(jnp.concatenate(rows + filler, axis=0))


def open_kernel(owners, shifts, wanted_ref, moments_ref, table_ref, counts_ref, terms_ref, *refs):
    message_refs, (high_ref, low_ref) = refs[: len(shifts)], refs[len(shifts) :]
    terms = tally(wanted_ref[...], moments_ref, high_ref, low_ref, counts_ref)
    terms_ref[...] = terms
    columns = asked_of_me(owners, wanted_ref, shifts)
    for place, message_ref in enumerate(message_refs):
        put(message_ref, pick(table_ref, columns[:, place : place + 1]), terms)


def serve_kernel(owners, shifts, wanted_ref, terms_ref, table_ref, *message_refs):
    columns = asked_of_me(owners, wanted_ref, shifts)
    for place, message_ref in enumerate(message_refs):
        put(message_ref, pick(table_ref, columns[:, place : place + 1]), terms_ref[...])


def serve_all_kernel(slot_count, mine_ref, wanted_ref, moments_ref, table_ref, payload_ref, counts_ref, high_ref, low_ref):
    pieces = table_ref.shape[1] // LANES
    terms = tally(wanted_ref[...], moments_ref, high_ref, low_ref, counts_ref)
    mine = jnp.transpose(mine_ref[...])
    for row in range(mine.shape[1]):
        rows = pick(table_ref, mine[:, row : row + 1]).astype(jnp.float32)
        for start in range(0, LANES, slot_count):
            peer = (row * LANES + start) // slot_count
            for piece in range(pieces):
                payload_ref[peer, piece * slot_count : (piece + 1) * slot_count, :] = rows[
                    start : start + slot_count, piece * LANES : (piece + 1) * LANES
                ].astype(jnp.bfloat16)
    for peer in range(payload_ref.shape[0]):
        payload_ref[peer, pieces * slot_count :, :] = terms


def merge(figures, moments_ref):
    counts = figures[:, 0:1]
    entries = jnp.sum(counts, axis=0, keepdims=True)
    whole = jnp.sum(counts * figures, axis=0, keepdims=True) / entries
    apart = jnp.sum(WIDTH * counts * jnp.square(figures - whole), axis=0, keepdims=True)
    within = jnp.sum(figures, axis=0, keepdims=True)
    out_row = lax.broadcasted_iota(jnp.int32, moments_ref.shape, 0)
    out_lane = lax.broadcasted_iota(jnp.int32, moments_ref.shape, 1)
    summary = jnp.zeros(moments_ref.shape, jnp.float32)
    means, scales = [], []
    for layer in range(LAYERS):
        at, beyond = 1 + layer, 1 + LAYERS + layer
        mean = whole[:, at : at + 1]
        variance = (apart[:, at : at + 1] + within[:, beyond : beyond + 1]) / (entries * WIDTH)
        means.append(mean)
        scales.append(lax.rsqrt(variance + epsilon))
        summary = jnp.where(out_lane == layer, jnp.where(out_row == 0, mean, variance), summary)
    moments_ref[...] = summary
    return means, scales


def normalize_kernel(order, used_ref, gain_ref, *refs):
    sources = refs[: -5]
    out_ref, moments_ref, figures_ref, ready_ref, sems = refs[-5:]
    owners, slot_count, columns = out_ref.shape
    pieces = columns // LANES
    blocks = order(sources)
    for owner, block_ref in blocks:
        terms = block_ref[pieces * slot_count :, :].astype(jnp.float32)
        figures_ref[pl.ds(owner, 1), :] = terms[0:1] + terms[1:2] + terms[2:3]
    means, scales = merge(figures_ref[...], moments_ref)
    slot = lax.broadcasted_iota(jnp.int32, (slot_count, LANES), 0)
    shift, factor = [], []
    for piece in range(pieces):
        layer = piece * LANES // WIDTH
        shift.append(jnp.broadcast_to(means[layer], (1, LANES)))
        factor.append(scales[layer] * gain_ref[:, piece * LANES : (piece + 1) * LANES])
    copies = []
    for place, (owner, block_ref) in enumerate(blocks):
        live = slot < used_ref[0, owner]
        for piece in range(pieces):
            x = block_ref[piece * slot_count : (piece + 1) * slot_count, :].astype(jnp.float32)
            ready_ref[place, :, piece * LANES : (piece + 1) * LANES] = jnp.where(
                live, (x - shift[piece]) * factor[piece], 0.0
            ).astype(jnp.bfloat16)
        copy = pltpu.make_async_copy(ready_ref.at[place], out_ref.at[owner], sems.at[place])
        copy.start()
        copies.append(copy)
    for copy in copies:
        copy.wait()


def normalize(order, request_counts, gain, sources, owners, slot_count):
    columns = gain.shape[0]
    return kernel_call(
        functools.partial(normalize_kernel, order),
        "normalize",
        (
            jax.ShapeDtypeStruct((owners, slot_count, columns), jnp.bfloat16),
            jax.ShapeDtypeStruct((2, LAYERS), jnp.float32),
        ),
        [SMEM] + [VMEM] * (1 + len(sources)),
        (PLACED, VMEM),
        (
            pltpu.VMEM((owners, LANES), jnp.float32),
            pltpu.VMEM((owners, slot_count, columns), jnp.bfloat16),
            pltpu.SemaphoreType.DMA((owners,)),
        ),
    )(request_counts, gain[None], *sources)


def by_shift(shifts, sources):
    owners = len(shifts)
    me = lax.axis_index("rows")
    return [(lax.rem(me + owners - shift, owners), ref) for shift, ref in zip(shifts, sources)]


def by_owner(sources):
    (received_ref,) = sources
    return [(owner, received_ref.at[owner]) for owner in range(received_ref.shape[0])]


def shifts_of(owners):
    return sorted(range(1, owners), key=lambda shift: (abs(shift - owners // 2), shift)) + [0]


def per_device(groups, requests, request_counts, table, gain):
    _, owners, slot_count = requests.shape
    held_rows, columns = table.shape
    pieces, blocks = columns // LANES, held_rows // LANES
    message_rows = pieces * slot_count + SUBLANES
    by_permutes = slot_count == LANES and owners <= MOST_PERMUTES
    moments = kernel_call(
        row_moments_kernel,
        "row_moments",
        jax.ShapeDtypeStruct((2 * LAYERS * blocks, LANES), jnp.float32),
        [VMEM],
        VMEM,
    )(table)
    if by_permutes:
        asked = kernel_call(
            functools.partial(ask_kernel, held_rows, groups),
            "ask",
            jax.ShapeDtypeStruct((groups * owners, slot_count), jnp.int32),
            [SMEM, VMEM],
            VMEM,
        )(request_counts, requests[0])
    else:
        slot = lax.broadcasted_iota(jnp.int32, (owners, slot_count), 1)
        asked = jnp.where(slot < request_counts[0][:, None], requests[0], held_rows)
        asked = jnp.broadcast_to(asked[None], (groups, owners, slot_count)).reshape(groups * owners, slot_count)
    wanted = lax.all_to_all(asked, ("rep", "rows"), split_axis=0, concat_axis=0, tiled=True)
    wanted = wanted.reshape(-1, LANES)
    counts_shape = jax.ShapeDtypeStruct((blocks, LANES), jnp.int32)
    tally_scratch = (
        pltpu.VMEM((blocks, wanted.size), jnp.bfloat16),
        pltpu.VMEM((wanted.size, LANES), jnp.bfloat16),
    )
    if by_permutes:
        message = jax.ShapeDtypeStruct((message_rows, LANES), jnp.bfloat16)
        shifts = shifts_of(owners)
        early, late = shifts[:1], shifts[1:]
        row_counts, terms, *messages = kernel_call(
            functools.partial(open_kernel, owners, early),
            "open",
            (counts_shape, jax.ShapeDtypeStruct((SUBLANES, LANES), jnp.bfloat16)) + (message,) * len(early),
            [VMEM] * 3,
            (VMEM,) * (2 + len(early)),
            tally_scratch,
        )(wanted, moments, table)
        messages += kernel_call(
            functools.partial(serve_kernel, owners, late),
            "serve",
            (message,) * len(late),
            [VMEM] * 3,
            (VMEM,) * len(late),
        )(wanted, terms, table)
        sources = [
            lax.ppermute(a, "rows", [(i, (i + shift) % owners) for i in range(owners)]) if shift else a
            for shift, a in zip(shifts, messages)
        ]
        order = functools.partial(by_shift, shifts)
    else:
        mine = lax.dynamic_index_in_dim(
            wanted.reshape(groups, -1, LANES), lax.axis_index("rep"), 0, False
        )
        payload, row_counts = kernel_call(
            functools.partial(serve_all_kernel, slot_count),
            "serve_all",
            (jax.ShapeDtypeStruct((owners, message_rows, LANES), jnp.bfloat16), counts_shape),
            [VMEM] * 4,
            (VMEM, VMEM),
            tally_scratch,
        )(mine, wanted, moments, table)
        sources = [lax.all_to_all(payload, "rows", split_axis=0, concat_axis=0, tiled=True)]
        order = by_owner
    normalized, summary = normalize(order, request_counts, gain, sources, owners, slot_count)
    return (normalized[None], row_counts.reshape(-1), summary)


def solution(mesh):
    return jax.shard_map(
        functools.partial(per_device, mesh.shape["rep"]),
        mesh=mesh,
        in_specs=(P(("rows", "rep"), None, None), P(("rows", "rep"), None), P("rows", None), P()),
        out_specs=(P(("rows", "rep"), None, None, None), P("rows"), P()),
        check_vma=False,
    )
```

```python
import functools

import jax
import jax.numpy as jnp
from jax import lax
from jax.experimental import pallas as pl
from jax.experimental.pallas import tpu as pltpu
from jax.sharding import PartitionSpec as P


WIDTH = 256
LAYERS = 2
LANES = 128
SUBLANES = 8
GRANT = 16 << 20
MOST_PERMUTES = 16

epsilon = 1e-06


VMEM = pl.BlockSpec(memory_space=pltpu.VMEM)
SMEM = pl.BlockSpec(memory_space=pltpu.SMEM)
PLACED = pl.BlockSpec(memory_space=pl.ANY)


def total(a):
    return jnp.sum(jnp.sum(a, axis=1, keepdims=True), axis=0, keepdims=True)


def one_hot(match):
    return jnp.where(match, 1.0, 0.0).astype(jnp.bfloat16)


def kernel_call(body, out_shape, in_specs, out_specs, scratch=()):
    return pl.pallas_call(
        body,
        out_shape=out_shape,
        in_specs=in_specs,
        out_specs=out_specs,
        scratch_shapes=list(scratch),
        compiler_params=pltpu.CompilerParams(vmem_limit_bytes=GRANT),
    )


def row_moments_kernel(table_ref, moments_ref):
    blocks = table_ref.shape[0] // LANES
    lane = lax.broadcasted_iota(jnp.int32, (LANES, LANES), 1)
    columns = jnp.zeros((LANES, LANES), jnp.float32)
    for block in range(blocks):
        for layer in range(LAYERS):
            x = table_ref[
                block * LANES : (block + 1) * LANES, layer * WIDTH : (layer + 1) * WIDTH
            ].astype(jnp.float32)
            mean = jnp.sum(x, axis=1, keepdims=True) * (1.0 / WIDTH)
            square = jnp.sum(jnp.square(x - mean), axis=1, keepdims=True)
            columns = jnp.where(lane == layer * blocks + block, mean, columns)
            columns = jnp.where(lane == (LAYERS + layer) * blocks + block, square, columns)
    moments_ref[...] = jnp.transpose(columns)[: 2 * LAYERS * blocks]


def tally(wanted, moments_ref, high_ref, low_ref, counts_ref):
    blocks = counts_ref.shape[0]
    lane = lax.broadcasted_iota(jnp.int32, (LANES, LANES), 1)
    block_row = lax.broadcasted_iota(jnp.int32, (blocks, LANES), 0)
    upright = jnp.transpose(wanted)
    for row in range(wanted.shape[0]):
        span = slice(row * LANES, (row + 1) * LANES)
        high_ref[:, span] = one_hot(block_row == wanted[row : row + 1] // LANES)
        low_ref[span, :] = one_hot(lane == upright[:, row : row + 1] % LANES)
    weights = jnp.dot(high_ref[...], low_ref[...], preferred_element_type=jnp.float32)
    counts_ref[...] = weights.astype(jnp.int32)

    tile_row = lax.broadcasted_iota(jnp.int32, (SUBLANES, LANES), 0)
    tile_lane = lax.broadcasted_iota(jnp.int32, (SUBLANES, LANES), 1)
    count = total(weights)
    figures = jnp.where(tile_lane == 0, count, 0.0)
    for layer in range(LAYERS):
        row_mean = moments_ref[layer * blocks : (layer + 1) * blocks]
        row_square = moments_ref[(LAYERS + layer) * blocks : (LAYERS + layer + 1) * blocks]
        mean = total(weights * row_mean) / jnp.maximum(count, 1.0)
        square = total(weights * (row_square + WIDTH * jnp.square(row_mean - mean)))
        figures = jnp.where(tile_lane == 1 + layer, mean, figures)
        figures = jnp.where(tile_lane == 1 + LAYERS + layer, square, figures)
    first = figures.astype(jnp.bfloat16).astype(jnp.float32)
    second = (figures - first).astype(jnp.bfloat16).astype(jnp.float32)
    third = figures - first - second
    return jnp.where(tile_row == 0, first, jnp.where(tile_row == 1, second, third)).astype(jnp.bfloat16)


def pick(table_ref, column):
    lane = lax.broadcasted_iota(jnp.int32, (LANES, table_ref.shape[0]), 1)
    return jnp.dot(one_hot(lane == column), table_ref[...], preferred_element_type=jnp.float32).astype(jnp.bfloat16)


def put(message_ref, rows, terms=None):
    count, columns = rows.shape
    pieces = columns // LANES
    for piece in range(pieces):
        message_ref[piece * count : (piece + 1) * count, :] = rows[:, piece * LANES : (piece + 1) * LANES]
    if terms is not None:
        message_ref[pieces * count :, :] = terms


def asked_of_me(owners, wanted_ref, shifts):
    me, group = lax.axis_index("rows"), lax.axis_index("rep")
    rows = [wanted_ref[pl.ds(group * owners + lax.rem(me + shift, owners), 1), :] for shift in shifts]
    filler = [rows[0]] * (-len(rows) % SUBLANES)
    return jnp.transpose(jnp.concatenate(rows + filler, axis=0))


def first_kernel(owners, shifts, wanted_ref, table_ref, passed_ref, *message_refs):
    passed_ref[...] = wanted_ref[...]
    columns = asked_of_me(owners, wanted_ref, shifts)
    for place, message_ref in enumerate(message_refs):
        put(message_ref, pick(table_ref, columns[:, place : place + 1]))


def tally_kernel(wanted_ref, moments_ref, counts_ref, terms_ref, high_ref, low_ref):
    terms_ref[...] = tally(wanted_ref[...], moments_ref, high_ref, low_ref, counts_ref)


def serve_kernel(owners, shifts, wanted_ref, terms_ref, table_ref, *message_refs):
    columns = asked_of_me(owners, wanted_ref, shifts)
    for place, message_ref in enumerate(message_refs):
        put(message_ref, pick(table_ref, columns[:, place : place + 1]), terms_ref[...])


def serve_all_kernel(slot_count, mine_ref, wanted_ref, moments_ref, table_ref, payload_ref, counts_ref, high_ref, low_ref):
    pieces = table_ref.shape[1] // LANES
    terms = tally(wanted_ref[...], moments_ref, high_ref, low_ref, counts_ref)
    mine = jnp.transpose(mine_ref[...])
    for row in range(mine.shape[1]):
        rows = pick(table_ref, mine[:, row : row + 1]).astype(jnp.float32)
        for start in range(0, LANES, slot_count):
            peer = (row * LANES + start) // slot_count
            for piece in range(pieces):
                payload_ref[peer, piece * slot_count : (piece + 1) * slot_count, :] = rows[
                    start : start + slot_count, piece * LANES : (piece + 1) * LANES
                ].astype(jnp.bfloat16)
    for peer in range(payload_ref.shape[0]):
        payload_ref[peer, pieces * slot_count :, :] = terms


def merge(figures, moments_ref):
    counts = figures[:, 0:1]
    entries = jnp.sum(counts, axis=0, keepdims=True)
    whole = jnp.sum(counts * figures, axis=0, keepdims=True) / entries
    apart = jnp.sum(WIDTH * counts * jnp.square(figures - whole), axis=0, keepdims=True)
    within = jnp.sum(figures, axis=0, keepdims=True)
    out_row = lax.broadcasted_iota(jnp.int32, moments_ref.shape, 0)
    out_lane = lax.broadcasted_iota(jnp.int32, moments_ref.shape, 1)
    summary = jnp.zeros(moments_ref.shape, jnp.float32)
    means, scales = [], []
    for layer in range(LAYERS):
        at, beyond = 1 + layer, 1 + LAYERS + layer
        mean = whole[:, at : at + 1]
        variance = (apart[:, at : at + 1] + within[:, beyond : beyond + 1]) / (entries * WIDTH)
        means.append(mean)
        scales.append(lax.rsqrt(variance + epsilon))
        summary = jnp.where(out_lane == layer, jnp.where(out_row == 0, mean, variance), summary)
    moments_ref[...] = summary
    return means, scales


def normalize_kernel(order, used_ref, gain_ref, *refs):
    sources = refs[: -5]
    out_ref, moments_ref, figures_ref, ready_ref, sems = refs[-5:]
    _, slot_count, columns = out_ref.shape
    pieces = columns // LANES
    blocks = order(sources)
    for owner, block_ref, terms_ref in blocks:
        terms = (block_ref[pieces * slot_count :, :] if terms_ref is None else terms_ref[...]).astype(jnp.float32)
        figures_ref[pl.ds(owner, 1), :] = terms[0:1] + terms[1:2] + terms[2:3]
    means, scales = merge(figures_ref[...], moments_ref)
    slot = lax.broadcasted_iota(jnp.int32, (slot_count, LANES), 0)
    shift, factor = [], []
    for piece in range(pieces):
        layer = piece * LANES // WIDTH
        shift.append(jnp.broadcast_to(means[layer], (1, LANES)))
        factor.append(scales[layer] * gain_ref[:, piece * LANES : (piece + 1) * LANES])
    copies = []
    for place, (owner, block_ref, _) in enumerate(blocks):
        live = slot < used_ref[0, owner]
        for piece in range(pieces):
            x = block_ref[piece * slot_count : (piece + 1) * slot_count, :].astype(jnp.float32)
            ready_ref[place, :, piece * LANES : (piece + 1) * LANES] = jnp.where(
                live, (x - shift[piece]) * factor[piece], 0.0
            ).astype(jnp.bfloat16)
        copy = pltpu.make_async_copy(ready_ref.at[place], out_ref.at[owner], sems.at[place])
        copy.start()
        copies.append(copy)
    for copy in copies:
        copy.wait()


def normalize(order, request_counts, gain, sources, owners, slot_count):
    columns = gain.shape[0]
    return kernel_call(
        functools.partial(normalize_kernel, order),
        (
            jax.ShapeDtypeStruct((owners, slot_count, columns), jnp.bfloat16),
            jax.ShapeDtypeStruct((2, LAYERS), jnp.float32),
        ),
        [SMEM] + [VMEM] * (1 + len(sources)),
        (PLACED, VMEM),
        (
            pltpu.VMEM((owners, LANES), jnp.float32),
            pltpu.VMEM((owners, slot_count, columns), jnp.bfloat16),
            pltpu.SemaphoreType.DMA((owners,)),
        ),
    )(request_counts, gain[None], *sources)


def by_shift(shifts, early, sources):
    owners = len(shifts)
    me = lax.axis_index("rows")
    apart = list(sources[owners:]) + [None] * (owners - early)
    return [
        (lax.rem(me + owners - shift, owners), block_ref, terms_ref)
        for shift, block_ref, terms_ref in zip(shifts, sources[:owners], apart)
    ]


def by_owner(sources):
    (received_ref,) = sources
    return [(owner, received_ref.at[owner], None) for owner in range(received_ref.shape[0])]


def shifts_of(owners):
    return sorted(range(1, owners), key=lambda shift: (abs(shift - owners // 2), shift)) + [0]


def per_device(groups, requests, request_counts, table, gain):
    _, owners, slot_count = requests.shape
    held_rows, columns = table.shape
    pieces, blocks = columns // LANES, held_rows // LANES
    bare = jax.ShapeDtypeStruct((pieces * slot_count, LANES), jnp.bfloat16)
    message = jax.ShapeDtypeStruct((pieces * slot_count + SUBLANES, LANES), jnp.bfloat16)
    figures = jax.ShapeDtypeStruct((SUBLANES, LANES), jnp.bfloat16)
    counts = jax.ShapeDtypeStruct((blocks, LANES), jnp.int32)
    everywhere = (groups, owners, slot_count)
    slot = lax.broadcasted_iota(jnp.int32, everywhere, 2)
    outside = held_rows + lax.broadcasted_iota(jnp.int32, everywhere, 0)
    asked = jnp.where(slot < request_counts[0][None, :, None], requests[0][None], outside)
    wanted = lax.all_to_all(
        asked.reshape(groups * owners, slot_count), ("rep", "rows"), split_axis=0, concat_axis=0, tiled=True
    ).reshape(-1, LANES)
    moments = kernel_call(
        row_moments_kernel, jax.ShapeDtypeStruct((2 * LAYERS * blocks, LANES), jnp.float32), [VMEM], VMEM
    )(table)
    tally_scratch = (
        pltpu.VMEM((blocks, wanted.size), jnp.bfloat16),
        pltpu.VMEM((wanted.size, LANES), jnp.bfloat16),
    )
    if slot_count == LANES and owners <= MOST_PERMUTES // 2:
        shifts = shifts_of(owners)
        early = 1

        def send(a, shift):
            if not shift:
                return a
            return lax.ppermute(a, "rows", [(i, (i + shift) % owners) for i in range(owners)])

        wanted, *first = kernel_call(
            functools.partial(first_kernel, owners, shifts[:early]),
            (jax.ShapeDtypeStruct(wanted.shape, jnp.int32),) + (bare,) * early,
            [VMEM] * 2,
            (VMEM,) * (1 + early),
        )(wanted, table)
        sources = [send(a, shift) for a, shift in zip(first, shifts)]
        row_counts, terms = kernel_call(
            tally_kernel, (counts, figures), [VMEM] * 2, (VMEM,) * 2, tally_scratch
        )(wanted, moments)
        rest = kernel_call(
            functools.partial(serve_kernel, owners, shifts[early:]),
            (message,) * (owners - early),
            [VMEM] * 3,
            (VMEM,) * (owners - early),
        )(wanted, terms, table)
        sources += [send(a, shift) for a, shift in zip(rest, shifts[early:])]
        sources += [send(terms, shift) for shift in shifts[:early]]
        order = functools.partial(by_shift, shifts, early)
    else:
        mine = lax.dynamic_index_in_dim(
            wanted.reshape(groups, -1, LANES), lax.axis_index("rep"), 0, False
        )
        payload, row_counts = kernel_call(
            functools.partial(serve_all_kernel, slot_count),
            (jax.ShapeDtypeStruct((owners,) + message.shape, jnp.bfloat16), counts),
            [VMEM] * 4,
            (VMEM, VMEM),
            tally_scratch,
        )(mine, wanted, moments, table)
        sources = [lax.all_to_all(payload, "rows", split_axis=0, concat_axis=0, tiled=True)]
        order = by_owner
    normalized, summary = normalize(order, request_counts, gain, sources, owners, slot_count)
    return (normalized[None], row_counts.reshape(-1), summary)


def solution(mesh):
    return jax.shard_map(
        functools.partial(per_device, mesh.shape["rep"]),
        mesh=mesh,
        in_specs=(P(("rows", "rep"), None, None), P(("rows", "rep"), None), P("rows", None), P()),
        out_specs=(P(("rows", "rep"), None, None, None), P("rows"), P()),
        check_vma=False,
    )
```

```python
import functools

import jax
import jax.numpy as jnp
from jax import lax
from jax.experimental import pallas as pl
from jax.experimental.pallas import tpu as pltpu
from jax.sharding import PartitionSpec as P


WIDTH = 256
LAYERS = 2
LANES = 128
SUBLANES = 8
GRANT = 16 << 20
WIDE_GRANT = 60 << 20
MOST_PERMUTES = 16

epsilon = 1e-06


VMEM = pl.BlockSpec(memory_space=pltpu.VMEM)
PLACED = pl.BlockSpec(memory_space=pl.ANY)
HBM = pl.BlockSpec(memory_space=pltpu.HBM)


def total(a):
    return jnp.sum(jnp.sum(a, axis=1, keepdims=True), axis=0, keepdims=True)


def one_hot(match):
    return jnp.where(match, 1.0, 0.0).astype(jnp.bfloat16)


def kernel_call(body, out_shape, in_specs, out_specs, scratch=(), grant=GRANT):
    return pl.pallas_call(
        body,
        out_shape=out_shape,
        in_specs=in_specs,
        out_specs=out_specs,
        scratch_shapes=list(scratch),
        compiler_params=pltpu.CompilerParams(vmem_limit_bytes=grant),
    )


def row_moments_kernel(table_ref, gain_ref, moments_ref, kept_gain_ref):
    kept_gain_ref[...] = gain_ref[...]
    blocks = table_ref.shape[0] // LANES
    lane = lax.broadcasted_iota(jnp.int32, (LANES, LANES), 1)
    columns = jnp.zeros((LANES, LANES), jnp.float32)
    for block in range(blocks):
        for layer in range(LAYERS):
            x = table_ref[
                block * LANES : (block + 1) * LANES, layer * WIDTH : (layer + 1) * WIDTH
            ].astype(jnp.float32)
            mean = jnp.sum(x, axis=1, keepdims=True) * (1.0 / WIDTH)
            square = jnp.sum(jnp.square(x - mean), axis=1, keepdims=True)
            columns = jnp.where(lane == layer * blocks + block, mean, columns)
            columns = jnp.where(lane == (LAYERS + layer) * blocks + block, square, columns)
    moments_ref[...] = jnp.transpose(columns)[: 2 * LAYERS * blocks]


def ask_kernel(held_rows, used_hbm, requests_hbm, everywhere_hbm, used_ref, requests_ref, asked_ref, sems):
    owners, slot_count = requests_ref.shape
    copies = [
        pltpu.make_async_copy(used_hbm, used_ref, sems.at[0]),
        pltpu.make_async_copy(requests_hbm, requests_ref, sems.at[1]),
    ]
    for copy in copies:
        copy.start()
    row = lax.broadcasted_iota(jnp.int32, (owners, slot_count), 0)
    slot = lax.broadcasted_iota(jnp.int32, (owners, slot_count), 1)
    copies[0].wait()
    used = jnp.zeros((owners, slot_count), jnp.int32)
    for owner in range(owners):
        used = jnp.where(row == owner, used_ref[0, owner], used)
    copies[1].wait()
    asked_ref[...] = jnp.where(slot < used, requests_ref[...], held_rows)
    copies = []
    for group in range(everywhere_hbm.shape[0]):
        copies.append(pltpu.make_async_copy(asked_ref, everywhere_hbm.at[group], sems.at[2 + group]))
        copies[-1].start()
    for copy in copies:
        copy.wait()


def tally(wanted, moments_ref, high_ref, low_ref, counts_ref):
    blocks = counts_ref.shape[0]
    lane = lax.broadcasted_iota(jnp.int32, (LANES, LANES), 1)
    block_row = lax.broadcasted_iota(jnp.int32, (blocks, LANES), 0)
    upright = jnp.transpose(wanted)
    for row in range(wanted.shape[0]):
        span = slice(row * LANES, (row + 1) * LANES)
        high_ref[:, span] = one_hot(block_row == wanted[row : row + 1] // LANES)
        low_ref[span, :] = one_hot(lane == upright[:, row : row + 1] % LANES)
    weights = jnp.dot(high_ref[...], low_ref[...], preferred_element_type=jnp.float32)
    counts_ref[...] = weights.astype(jnp.int32)

    tile_row = lax.broadcasted_iota(jnp.int32, (SUBLANES, LANES), 0)
    tile_lane = lax.broadcasted_iota(jnp.int32, (SUBLANES, LANES), 1)
    count = total(weights)
    figures = jnp.where(tile_lane == 0, count, 0.0)
    for layer in range(LAYERS):
        row_mean = moments_ref[layer * blocks : (layer + 1) * blocks]
        row_square = moments_ref[(LAYERS + layer) * blocks : (LAYERS + layer + 1) * blocks]
        mean = total(weights * row_mean) / jnp.maximum(count, 1.0)
        square = total(weights * (row_square + WIDTH * jnp.square(row_mean - mean)))
        figures = jnp.where(tile_lane == 1 + layer, mean, figures)
        figures = jnp.where(tile_lane == 1 + LAYERS + layer, square, figures)
    first = figures.astype(jnp.bfloat16).astype(jnp.float32)
    second = (figures - first).astype(jnp.bfloat16).astype(jnp.float32)
    third = figures - first - second
    return jnp.where(tile_row == 0, first, jnp.where(tile_row == 1, second, third)).astype(jnp.bfloat16)


def pick(table_ref, column):
    lane = lax.broadcasted_iota(jnp.int32, (LANES, table_ref.shape[0]), 1)
    return jnp.dot(one_hot(lane == column), table_ref[...], preferred_element_type=jnp.float32).astype(jnp.bfloat16)


def put(message_ref, rows, terms=None):
    count, columns = rows.shape
    pieces = columns // LANES
    for piece in range(pieces):
        message_ref[piece * count : (piece + 1) * count, :] = rows[:, piece * LANES : (piece + 1) * LANES]
    if terms is not None:
        message_ref[pieces * count :, :] = terms


def asked_of_me(owners, wanted_ref, shifts):
    me, group = lax.axis_index("rows"), lax.axis_index("rep")
    rows = [wanted_ref[pl.ds(group * owners + lax.rem(me + shift, owners), 1), :] for shift in shifts]
    filler = [rows[0]] * (-len(rows) % SUBLANES)
    return jnp.transpose(jnp.concatenate(rows + filler, axis=0))


def first_kernel(owners, shifts, wanted_ref, table_ref, passed_ref, *message_refs):
    passed_ref[...] = wanted_ref[...]
    columns = asked_of_me(owners, wanted_ref, shifts)
    for place, message_ref in enumerate(message_refs):
        put(message_ref, pick(table_ref, columns[:, place : place + 1]))


def tally_kernel(wanted_ref, moments_ref, counts_ref, terms_ref, high_ref, low_ref):
    terms_ref[...] = tally(wanted_ref[...], moments_ref, high_ref, low_ref, counts_ref)


def serve_kernel(owners, shifts, wanted_ref, terms_ref, table_ref, *message_refs):
    columns = asked_of_me(owners, wanted_ref, shifts)
    for place, message_ref in enumerate(message_refs):
        put(message_ref, pick(table_ref, columns[:, place : place + 1]), terms_ref[...])


def serve_all_kernel(slot_count, mine_ref, wanted_ref, moments_ref, table_ref, payload_ref, counts_ref, high_ref, low_ref):
    pieces = table_ref.shape[1] // LANES
    terms = tally(wanted_ref[...], moments_ref, high_ref, low_ref, counts_ref)
    mine = jnp.transpose(mine_ref[...])
    for row in range(mine.shape[1]):
        rows = pick(table_ref, mine[:, row : row + 1]).astype(jnp.float32)
        for start in range(0, LANES, slot_count):
            peer = (row * LANES + start) // slot_count
            for piece in range(pieces):
                payload_ref[peer, piece * slot_count : (piece + 1) * slot_count, :] = rows[
                    start : start + slot_count, piece * LANES : (piece + 1) * LANES
                ].astype(jnp.bfloat16)
    for peer in range(payload_ref.shape[0]):
        payload_ref[peer, pieces * slot_count :, :] = terms


def merge(figures, moments_ref):
    counts = figures[:, 0:1]
    entries = jnp.sum(counts, axis=0, keepdims=True)
    whole = jnp.sum(counts * figures, axis=0, keepdims=True) / entries
    apart = jnp.sum(WIDTH * counts * jnp.square(figures - whole), axis=0, keepdims=True)
    within = jnp.sum(figures, axis=0, keepdims=True)
    out_row = lax.broadcasted_iota(jnp.int32, moments_ref.shape, 0)
    out_lane = lax.broadcasted_iota(jnp.int32, moments_ref.shape, 1)
    summary = jnp.zeros(moments_ref.shape, jnp.float32)
    means, scales = [], []
    for layer in range(LAYERS):
        at, beyond = 1 + layer, 1 + LAYERS + layer
        mean = whole[:, at : at + 1]
        variance = (apart[:, at : at + 1] + within[:, beyond : beyond + 1]) / (entries * WIDTH)
        means.append(mean)
        scales.append(lax.rsqrt(variance + epsilon))
        summary = jnp.where(out_lane == layer, jnp.where(out_row == 0, mean, variance), summary)
    moments_ref[...] = summary
    return means, scales


def normalize_kernel(order, held_rows, asked_ref, gain_ref, tally_ref, *refs):
    sources = refs[:-8]
    out_ref, counts_ref, moments_ref, figures_ref, ready_ref, summary_ref, sems, other_sems = refs[-8:]
    owners, slot_count, columns = out_ref.shape
    pieces = columns // LANES
    copies = [pltpu.make_async_copy(tally_ref, counts_ref, other_sems.at[0])]
    copies[0].start()
    blocks = order(sources)
    for owner, block_ref, terms_ref in blocks:
        terms = (block_ref[pieces * slot_count :, :] if terms_ref is None else terms_ref[...]).astype(jnp.float32)
        figures_ref[pl.ds(owner, 1), :] = terms[0:1] + terms[1:2] + terms[2:3]
    means, scales = merge(figures_ref[...], summary_ref)
    copies.append(pltpu.make_async_copy(summary_ref, moments_ref, other_sems.at[1]))
    copies[1].start()
    asked = [asked_ref[pl.ds(owner, 1), :] for owner, _, _ in blocks]
    asked = jnp.transpose(jnp.concatenate(asked + asked[:1] * (-owners % SUBLANES), axis=0))
    shift, factor = [], []
    for piece in range(pieces):
        layer = piece * LANES // WIDTH
        shift.append(jnp.broadcast_to(means[layer], (1, LANES)))
        factor.append(scales[layer] * gain_ref[:, piece * LANES : (piece + 1) * LANES])
    for place, (owner, block_ref, _) in enumerate(blocks):
        live = asked[:, place : place + 1] < held_rows
        for piece in range(pieces):
            x = block_ref[piece * slot_count : (piece + 1) * slot_count, :].astype(jnp.float32)
            ready_ref[place, :, piece * LANES : (piece + 1) * LANES] = jnp.where(
                live, (x - shift[piece]) * factor[piece], 0.0
            ).astype(jnp.bfloat16)
        copies.append(pltpu.make_async_copy(ready_ref.at[place], out_ref.at[owner], sems.at[place]))
        copies[-1].start()
    for copy in copies:
        copy.wait()


def normalize(order, held_rows, asked, gain, tallied, sources):
    (owners, slot_count), columns = asked.shape, gain.shape[1]
    return kernel_call(
        functools.partial(normalize_kernel, order, held_rows),
        (
            jax.ShapeDtypeStruct((owners, slot_count, columns), jnp.bfloat16),
            jax.ShapeDtypeStruct(tallied.shape, jnp.int32),
            jax.ShapeDtypeStruct((2, LAYERS), jnp.float32),
        ),
        [VMEM] * (3 + len(sources)),
        (PLACED,) * 3,
        (
            pltpu.VMEM((owners, LANES), jnp.float32),
            pltpu.VMEM((owners, slot_count, columns), jnp.bfloat16),
            pltpu.VMEM((2, LAYERS), jnp.float32),
            pltpu.SemaphoreType.DMA((owners,)),
            pltpu.SemaphoreType.DMA((2,)),
        ),
    )(asked, gain, tallied, *sources)


def by_shift(shifts, early, sources):
    owners = len(shifts)
    me = lax.axis_index("rows")
    apart = list(sources[owners:]) + [None] * (owners - early)
    return [
        (lax.rem(me + owners - shift, owners), block_ref, terms_ref)
        for shift, block_ref, terms_ref in zip(shifts, sources[:owners], apart)
    ]


def by_owner(sources):
    (received_ref,) = sources
    return [(owner, received_ref.at[owner], None) for owner in range(received_ref.shape[0])]


def shifts_of(owners):
    return sorted(range(1, owners), key=lambda shift: (abs(shift - owners // 2), shift)) + [0]


def per_device(groups, requests, request_counts, table, gain):
    _, owners, slot_count = requests.shape
    held_rows, columns = table.shape
    pieces, blocks = columns // LANES, held_rows // LANES
    bare = jax.ShapeDtypeStruct((pieces * slot_count, LANES), jnp.bfloat16)
    message = jax.ShapeDtypeStruct((pieces * slot_count + SUBLANES, LANES), jnp.bfloat16)
    figures = jax.ShapeDtypeStruct((SUBLANES, LANES), jnp.bfloat16)
    counts = jax.ShapeDtypeStruct((blocks, LANES), jnp.int32)
    by_permutes = slot_count == LANES and owners <= MOST_PERMUTES // 2
    if by_permutes:
        everywhere = kernel_call(
            functools.partial(ask_kernel, held_rows),
            jax.ShapeDtypeStruct((groups, owners, slot_count), jnp.int32),
            [HBM] * 2,
            HBM,
            (
                pltpu.SMEM((1, owners), jnp.int32),
                pltpu.VMEM((owners, slot_count), jnp.int32),
                pltpu.VMEM((owners, slot_count), jnp.int32),
                pltpu.SemaphoreType.DMA((2 + groups,)),
            ),
            WIDE_GRANT,
        )(request_counts, requests[0])
        asked = everywhere[0]
    else:
        slot = lax.broadcasted_iota(jnp.int32, (owners, slot_count), 1)
        asked = jnp.where(slot < request_counts[0][:, None], requests[0], held_rows)
        everywhere = jnp.broadcast_to(asked[None], (groups, owners, slot_count))
    wanted = lax.all_to_all(
        everywhere.reshape(groups * owners, slot_count), ("rep", "rows"), split_axis=0, concat_axis=0, tiled=True
    ).reshape(-1, LANES)
    moments, gain = kernel_call(
        row_moments_kernel,
        (
            jax.ShapeDtypeStruct((2 * LAYERS * blocks, LANES), jnp.float32),
            jax.ShapeDtypeStruct((1, columns), jnp.float32),
        ),
        [VMEM] * 2,
        (VMEM,) * 2,
    )(table, gain[None])
    tally_scratch = (
        pltpu.VMEM((blocks, wanted.size), jnp.bfloat16),
        pltpu.VMEM((wanted.size, LANES), jnp.bfloat16),
    )
    if by_permutes:
        shifts = shifts_of(owners)
        early = 1

        def send(a, shift):
            if not shift:
                return a
            return lax.ppermute(a, "rows", [(i, (i + shift) % owners) for i in range(owners)])

        wanted, *first = kernel_call(
            functools.partial(first_kernel, owners, shifts[:early]),
            (jax.ShapeDtypeStruct(wanted.shape, jnp.int32),) + (bare,) * early,
            [VMEM] * 2,
            (VMEM,) * (1 + early),
        )(wanted, table)
        sources = [send(a, shift) for a, shift in zip(first, shifts)]
        tallied, terms = kernel_call(
            tally_kernel, (counts, figures), [VMEM] * 2, (VMEM,) * 2, tally_scratch
        )(wanted, moments)
        rest = kernel_call(
            functools.partial(serve_kernel, owners, shifts[early:]),
            (message,) * (owners - early),
            [VMEM] * 3,
            (VMEM,) * (owners - early),
        )(wanted, terms, table)
        sources += [send(a, shift) for a, shift in zip(rest, shifts[early:])]
        sources += [send(terms, shift) for shift in shifts[:early]]
        order = functools.partial(by_shift, shifts, early)
    else:
        mine = lax.dynamic_index_in_dim(
            wanted.reshape(groups, -1, LANES), lax.axis_index("rep"), 0, False
        )
        payload, tallied = kernel_call(
            functools.partial(serve_all_kernel, slot_count),
            (jax.ShapeDtypeStruct((owners,) + message.shape, jnp.bfloat16), counts),
            [VMEM] * 4,
            (VMEM, VMEM),
            tally_scratch,
        )(mine, wanted, moments, table)
        sources = [lax.all_to_all(payload, "rows", split_axis=0, concat_axis=0, tiled=True)]
        order = by_owner
    normalized, row_counts, summary = normalize(order, held_rows, asked, gain, tallied, sources)
    return (normalized[None], row_counts.reshape(-1), summary)


def solution(mesh):
    return jax.shard_map(
        functools.partial(per_device, mesh.shape["rep"]),
        mesh=mesh,
        in_specs=(P(("rows", "rep"), None, None), P(("rows", "rep"), None), P("rows", None), P()),
        out_specs=(P(("rows", "rep"), None, None, None), P("rows"), P()),
        check_vma=False,
    )
```

```python
import functools

import jax
import jax.numpy as jnp
from jax import lax
from jax.experimental import pallas as pl
from jax.experimental.pallas import tpu as pltpu
from jax.sharding import PartitionSpec as P


WIDTH = 256
LAYERS = 2
LANES = 128
SUBLANES = 8
GRANT = 16 << 20
WIDE_GRANT = 60 << 20
MOST_PERMUTES = 16
AHEAD = 1

epsilon = 1e-06


VMEM = pl.BlockSpec(memory_space=pltpu.VMEM)
PLACED = pl.BlockSpec(memory_space=pl.ANY)
HBM = pl.BlockSpec(memory_space=pltpu.HBM)


def total(a):
    return jnp.sum(jnp.sum(a, axis=1, keepdims=True), axis=0, keepdims=True)


def one_hot(match):
    return jnp.where(match, 1.0, 0.0).astype(jnp.bfloat16)


def kernel_call(body, out_shape, in_specs, out_specs, scratch=(), grant=GRANT):
    return pl.pallas_call(
        body,
        out_shape=out_shape,
        in_specs=in_specs,
        out_specs=out_specs,
        scratch_shapes=list(scratch),
        compiler_params=pltpu.CompilerParams(vmem_limit_bytes=grant),
    )


def row_moments_kernel(table_ref, gain_ref, moments_ref, kept_gain_ref):
    kept_gain_ref[...] = gain_ref[...]
    blocks = table_ref.shape[0] // LANES
    lane = lax.broadcasted_iota(jnp.int32, (LANES, LANES), 1)
    columns = jnp.zeros((LANES, LANES), jnp.float32)
    for block in range(blocks):
        for layer in range(LAYERS):
            x = table_ref[
                block * LANES : (block + 1) * LANES, layer * WIDTH : (layer + 1) * WIDTH
            ].astype(jnp.float32)
            mean = jnp.sum(x, axis=1, keepdims=True) * (1.0 / WIDTH)
            square = jnp.sum(jnp.square(x - mean), axis=1, keepdims=True)
            columns = jnp.where(lane == layer * blocks + block, mean, columns)
            columns = jnp.where(lane == (LAYERS + layer) * blocks + block, square, columns)
    moments_ref[...] = jnp.transpose(columns)[: 2 * LAYERS * blocks]


def ask_kernel(held_rows, used_hbm, requests_hbm, asked_hbm, everywhere_hbm, used_ref, requests_ref, asked_ref, sems):
    owners, slot_count = requests_ref.shape
    copies = [
        pltpu.make_async_copy(used_hbm, used_ref, sems.at[0]),
        pltpu.make_async_copy(requests_hbm, requests_ref, sems.at[1]),
    ]
    for copy in copies:
        copy.start()
    row = lax.broadcasted_iota(jnp.int32, (owners, slot_count), 0)
    slot = lax.broadcasted_iota(jnp.int32, (owners, slot_count), 1)
    copies[0].wait()
    used = jnp.zeros((owners, slot_count), jnp.int32)
    for owner in range(owners):
        used = jnp.where(row == owner, used_ref[0, owner], used)
    copies[1].wait()
    asked_ref[...] = jnp.where(slot < used, requests_ref[...], held_rows)
    copies = []
    for place, target in enumerate([asked_hbm] + [everywhere_hbm.at[group] for group in range(everywhere_hbm.shape[0])]):
        copies.append(pltpu.make_async_copy(asked_ref, target, sems.at[2 + place]))
        copies[-1].start()
    for copy in copies:
        copy.wait()


def tally(wanted, moments_ref, high_ref, low_ref, counts_ref):
    blocks = counts_ref.shape[0]
    lane = lax.broadcasted_iota(jnp.int32, (LANES, LANES), 1)
    block_row = lax.broadcasted_iota(jnp.int32, (blocks, LANES), 0)
    upright = jnp.transpose(wanted)
    for row in range(wanted.shape[0]):
        span = slice(row * LANES, (row + 1) * LANES)
        high_ref[:, span] = one_hot(block_row == wanted[row : row + 1] // LANES)
        low_ref[span, :] = one_hot(lane == upright[:, row : row + 1] % LANES)
    weights = jnp.dot(high_ref[...], low_ref[...], preferred_element_type=jnp.float32)
    counts_ref[...] = weights.astype(jnp.int32)

    tile_row = lax.broadcasted_iota(jnp.int32, (SUBLANES, LANES), 0)
    tile_lane = lax.broadcasted_iota(jnp.int32, (SUBLANES, LANES), 1)
    count = total(weights)
    figures = jnp.where(tile_lane == 0, count, 0.0)
    for layer in range(LAYERS):
        row_mean = moments_ref[layer * blocks : (layer + 1) * blocks]
        row_square = moments_ref[(LAYERS + layer) * blocks : (LAYERS + layer + 1) * blocks]
        mean = total(weights * row_mean) / jnp.maximum(count, 1.0)
        square = total(weights * (row_square + WIDTH * jnp.square(row_mean - mean)))
        figures = jnp.where(tile_lane == 1 + layer, mean, figures)
        figures = jnp.where(tile_lane == 1 + LAYERS + layer, square, figures)
    first = figures.astype(jnp.bfloat16).astype(jnp.float32)
    second = (figures - first).astype(jnp.bfloat16).astype(jnp.float32)
    third = figures - first - second
    return jnp.where(tile_row == 0, first, jnp.where(tile_row == 1, second, third)).astype(jnp.bfloat16)


def pick(table_ref, column):
    lane = lax.broadcasted_iota(jnp.int32, (LANES, table_ref.shape[0]), 1)
    return jnp.dot(one_hot(lane == column), table_ref[...], preferred_element_type=jnp.float32).astype(jnp.bfloat16)


def put(message_ref, rows, terms=None):
    count, columns = rows.shape
    pieces = columns // LANES
    for piece in range(pieces):
        message_ref[piece * count : (piece + 1) * count, :] = rows[:, piece * LANES : (piece + 1) * LANES]
    if terms is not None:
        message_ref[pieces * count :, :] = terms


def asked_of_me(owners, wanted_ref, shifts):
    me, group = lax.axis_index("rows"), lax.axis_index("rep")
    rows = [wanted_ref[pl.ds(group * owners + lax.rem(me + shift, owners), 1), :] for shift in shifts]
    filler = [rows[0]] * (-len(rows) % SUBLANES)
    return jnp.transpose(jnp.concatenate(rows + filler, axis=0))


def first_kernel(asked_ref, table_ref, message_ref):
    row = asked_ref[pl.ds(lax.axis_index("rows"), 1), :]
    column = jnp.transpose(jnp.concatenate([row] * SUBLANES, axis=0))[:, :1]
    put(message_ref, pick(table_ref, column))


def tally_kernel(wanted_ref, moments_ref, counts_ref, terms_ref, high_ref, low_ref):
    terms_ref[...] = tally(wanted_ref[...], moments_ref, high_ref, low_ref, counts_ref)


def serve_kernel(owners, shifts, wanted_ref, terms_ref, table_ref, *message_refs):
    columns = asked_of_me(owners, wanted_ref, shifts)
    for place, message_ref in enumerate(message_refs):
        put(message_ref, pick(table_ref, columns[:, place : place + 1]), terms_ref[...])


def serve_all_kernel(slot_count, mine_ref, wanted_ref, moments_ref, table_ref, payload_ref, counts_ref, high_ref, low_ref):
    pieces = table_ref.shape[1] // LANES
    terms = tally(wanted_ref[...], moments_ref, high_ref, low_ref, counts_ref)
    mine = jnp.transpose(mine_ref[...])
    for row in range(mine.shape[1]):
        rows = pick(table_ref, mine[:, row : row + 1]).astype(jnp.float32)
        for start in range(0, LANES, slot_count):
            peer = (row * LANES + start) // slot_count
            for piece in range(pieces):
                payload_ref[peer, piece * slot_count : (piece + 1) * slot_count, :] = rows[
                    start : start + slot_count, piece * LANES : (piece + 1) * LANES
                ].astype(jnp.bfloat16)
    for peer in range(payload_ref.shape[0]):
        payload_ref[peer, pieces * slot_count :, :] = terms


def merge(figures, moments_ref):
    counts = figures[:, 0:1]
    entries = jnp.sum(counts, axis=0, keepdims=True)
    whole = jnp.sum(counts * figures, axis=0, keepdims=True) / entries
    apart = jnp.sum(WIDTH * counts * jnp.square(figures - whole), axis=0, keepdims=True)
    within = jnp.sum(figures, axis=0, keepdims=True)
    out_row = lax.broadcasted_iota(jnp.int32, moments_ref.shape, 0)
    out_lane = lax.broadcasted_iota(jnp.int32, moments_ref.shape, 1)
    summary = jnp.zeros(moments_ref.shape, jnp.float32)
    means, scales = [], []
    for layer in range(LAYERS):
        at, beyond = 1 + layer, 1 + LAYERS + layer
        mean = whole[:, at : at + 1]
        variance = (apart[:, at : at + 1] + within[:, beyond : beyond + 1]) / (entries * WIDTH)
        means.append(mean)
        scales.append(lax.rsqrt(variance + epsilon))
        summary = jnp.where(out_lane == layer, jnp.where(out_row == 0, mean, variance), summary)
    moments_ref[...] = summary
    return means, scales


def normalize_kernel(order, held_rows, asked_ref, gain_ref, tally_ref, *refs):
    sources = refs[:-8]
    out_ref, counts_ref, moments_ref, figures_ref, ready_ref, summary_ref, sems, other_sems = refs[-8:]
    owners, slot_count, columns = out_ref.shape
    pieces = columns // LANES
    copies = [pltpu.make_async_copy(tally_ref, counts_ref, other_sems.at[0])]
    copies[0].start()
    blocks = order(sources)
    for owner, block_ref, terms_ref in blocks:
        terms = (block_ref[pieces * slot_count :, :] if terms_ref is None else terms_ref[...]).astype(jnp.float32)
        figures_ref[pl.ds(owner, 1), :] = terms[0:1] + terms[1:2] + terms[2:3]
    means, scales = merge(figures_ref[...], summary_ref)
    copies.append(pltpu.make_async_copy(summary_ref, moments_ref, other_sems.at[1]))
    copies[1].start()
    asked = [asked_ref[pl.ds(owner, 1), :] for owner, _, _ in blocks]
    asked = jnp.transpose(jnp.concatenate(asked + asked[:1] * (-owners % SUBLANES), axis=0))
    shift, factor = [], []
    for piece in range(pieces):
        layer = piece * LANES // WIDTH
        shift.append(jnp.broadcast_to(means[layer], (1, LANES)))
        factor.append(scales[layer] * gain_ref[:, piece * LANES : (piece + 1) * LANES])
    for place, (owner, block_ref, _) in enumerate(blocks):
        live = asked[:, place : place + 1] < held_rows
        for piece in range(pieces):
            x = block_ref[piece * slot_count : (piece + 1) * slot_count, :].astype(jnp.float32)
            ready_ref[place, :, piece * LANES : (piece + 1) * LANES] = jnp.where(
                live, (x - shift[piece]) * factor[piece], 0.0
            ).astype(jnp.bfloat16)
        copies.append(pltpu.make_async_copy(ready_ref.at[place], out_ref.at[owner], sems.at[place]))
        copies[-1].start()
    for copy in copies:
        copy.wait()


def normalize(order, held_rows, asked, gain, tallied, sources):
    (owners, slot_count), columns = asked.shape, gain.shape[1]
    return kernel_call(
        functools.partial(normalize_kernel, order, held_rows),
        (
            jax.ShapeDtypeStruct((owners, slot_count, columns), jnp.bfloat16),
            jax.ShapeDtypeStruct(tallied.shape, jnp.int32),
            jax.ShapeDtypeStruct((2, LAYERS), jnp.float32),
        ),
        [VMEM] * (3 + len(sources)),
        (PLACED,) * 3,
        (
            pltpu.VMEM((owners, LANES), jnp.float32),
            pltpu.VMEM((owners, slot_count, columns), jnp.bfloat16),
            pltpu.VMEM((2, LAYERS), jnp.float32),
            pltpu.SemaphoreType.DMA((owners,)),
            pltpu.SemaphoreType.DMA((2,)),
        ),
    )(asked, gain, tallied, *sources)


def by_shift(shifts, early, sources):
    owners = len(shifts)
    me = lax.axis_index("rows")
    apart = list(sources[owners:]) + [None] * (owners - early)
    return [
        (lax.rem(me + owners - shift, owners), block_ref, terms_ref)
        for shift, block_ref, terms_ref in zip(shifts, sources[:owners], apart)
    ]


def by_owner(sources):
    (received_ref,) = sources
    return [(owner, received_ref.at[owner], None) for owner in range(received_ref.shape[0])]


def shifts_of(owners):
    return sorted(range(1, owners), key=lambda shift: (abs(shift - owners // 2), shift)) + [0]


def per_device(groups, requests, request_counts, table, gain):
    _, owners, slot_count = requests.shape
    held_rows, columns = table.shape
    pieces, blocks = columns // LANES, held_rows // LANES
    bare = jax.ShapeDtypeStruct((pieces * slot_count, LANES), jnp.bfloat16)
    message = jax.ShapeDtypeStruct((pieces * slot_count + SUBLANES, LANES), jnp.bfloat16)
    figures = jax.ShapeDtypeStruct((SUBLANES, LANES), jnp.bfloat16)
    counts = jax.ShapeDtypeStruct((blocks, LANES), jnp.int32)
    by_permutes = slot_count == LANES and owners <= MOST_PERMUTES // 2
    if by_permutes:
        asked, everywhere = kernel_call(
            functools.partial(ask_kernel, held_rows),
            (
                jax.ShapeDtypeStruct((owners, slot_count), jnp.int32),
                jax.ShapeDtypeStruct((groups, owners, slot_count), jnp.int32),
            ),
            [HBM] * 2,
            (HBM,) * 2,
            (
                pltpu.SMEM((1, owners), jnp.int32),
                pltpu.VMEM((owners, slot_count), jnp.int32),
                pltpu.VMEM((owners, slot_count), jnp.int32),
                pltpu.SemaphoreType.DMA((3 + groups,)),
            ),
            WIDE_GRANT,
        )(request_counts, requests[0])
    else:
        slot = lax.broadcasted_iota(jnp.int32, (owners, slot_count), 1)
        asked = jnp.where(slot < request_counts[0][:, None], requests[0], held_rows)
        everywhere = jnp.broadcast_to(asked[None], (groups, owners, slot_count))
    wanted = lax.all_to_all(
        everywhere.reshape(groups * owners, slot_count), ("rep", "rows"), split_axis=0, concat_axis=0, tiled=True
    )
    wanted = wanted.reshape(-1, LANES)
    moments, gain = kernel_call(
        row_moments_kernel,
        (
            jax.ShapeDtypeStruct((2 * LAYERS * blocks, LANES), jnp.float32),
            jax.ShapeDtypeStruct((1, columns), jnp.float32),
        ),
        [VMEM] * 2,
        (VMEM,) * 2,
    )(table, gain[None])
    tally_scratch = (
        pltpu.VMEM((blocks, wanted.size), jnp.bfloat16),
        pltpu.VMEM((wanted.size, LANES), jnp.bfloat16),
    )
    if by_permutes:
        shifts = shifts_of(owners)

        def send(a, shift):
            if not shift:
                return a
            return lax.ppermute(a, "rows", [(i, (i + shift) % owners) for i in range(owners)])

        sources = []
        for shift in shifts[:AHEAD]:
            asked_first = send(asked, -shift)
            message_first = kernel_call(first_kernel, bare, [VMEM] * 2, VMEM)(asked_first, table)
            sources.append(send(message_first, shift))
        tallied, terms = kernel_call(
            tally_kernel, (counts, figures), [VMEM] * 2, (VMEM,) * 2, tally_scratch
        )(wanted, moments)
        rest = kernel_call(
            functools.partial(serve_kernel, owners, shifts[AHEAD:]),
            (message,) * (owners - AHEAD),
            [VMEM] * 3,
            (VMEM,) * (owners - AHEAD),
        )(wanted, terms, table)
        sources += [send(a, shift) for a, shift in zip(rest, shifts[AHEAD:])]
        sources += [send(terms, shift) for shift in shifts[:AHEAD]]
        order = functools.partial(by_shift, shifts, AHEAD)
    else:
        mine = lax.dynamic_index_in_dim(
            wanted.reshape(groups, -1, LANES), lax.axis_index("rep"), 0, False
        )
        payload, tallied = kernel_call(
            functools.partial(serve_all_kernel, slot_count),
            (jax.ShapeDtypeStruct((owners,) + message.shape, jnp.bfloat16), counts),
            [VMEM] * 4,
            (VMEM, VMEM),
            tally_scratch,
        )(mine, wanted, moments, table)
        sources = [lax.all_to_all(payload, "rows", split_axis=0, concat_axis=0, tiled=True)]
        order = by_owner
    normalized, row_counts, summary = normalize(order, held_rows, asked, gain, tallied, sources)
    return (normalized[None], row_counts.reshape(-1), summary)


def solution(mesh):
    return jax.shard_map(
        functools.partial(per_device, mesh.shape["rep"]),
        mesh=mesh,
        in_specs=(P(("rows", "rep"), None, None), P(("rows", "rep"), None), P("rows", None), P()),
        out_specs=(P(("rows", "rep"), None, None, None), P("rows"), P()),
        check_vma=False,
    )
```
